32 devices in a mesh: dp: 1 (over z), tp: 32 (over y, x, core).
Axes of the slice: x: 4, y: 4, z: 1, core: 2. Of those that a mesh axis runs over, the one named last changes fastest.
The devices are a block of a 4x4x8 slice.
Arguments:
- x_in: bfloat16 [8, 512, 4096], P('dp')
- adapter_ids: int32 [8], P('dp')
- gain_attn: float32 [4096], replicated
- gain_mlp: float32 [4096], replicated
- w_q: bfloat16 [4096, 32, 128], P(None, 'tp')
- w_k: bfloat16 [4096, 32, 128], P(None, 'tp')
- w_v: bfloat16 [4096, 32, 128], P(None, 'tp')
- w_o: bfloat16 [32, 128, 4096], P('tp')
- w_gate: bfloat16 [4096, 11008], P(None, 'tp')
- w_up: bfloat16 [4096, 11008], P(None, 'tp')
- w_down: bfloat16 [11008, 4096], P('tp')
- a_q: bfloat16 [4, 4096, 32], P(None, None, 'tp')
- b_q: bfloat16 [4, 32, 32, 128], P(None, None, 'tp')
- a_k: bfloat16 [4, 4096, 32], P(None, None, 'tp')
- b_k: bfloat16 [4, 32, 32, 128], P(None, None, 'tp')
- a_v: bfloat16 [4, 4096, 32], P(None, None, 'tp')
- b_v: bfloat16 [4, 32, 32, 128], P(None, None, 'tp')
- a_o: bfloat16 [4, 32, 128, 32], P(None, 'tp')
- b_o: bfloat16 [4, 32, 4096], P(None, None, 'tp')
- a_gate: bfloat16 [4, 4096, 32], P(None, None, 'tp')
- b_gate: bfloat16 [4, 32, 11008], P(None, None, 'tp')
- a_up: bfloat16 [4, 4096, 32], P(None, None, 'tp')
- b_up: bfloat16 [4, 32, 11008], P(None, None, 'tp')
- a_down: bfloat16 [4, 11008, 32], P(None, 'tp')
- b_down: bfloat16 [4, 32, 4096], P(None, None, 'tp')
Outputs:
- output: bfloat16 [8, 512, 4096], P('dp')
All inputs are finite; a program needn't handle non-finite values.
Results may differ from the reference program's by a relative error of at most 0.02.
Values are sent between devices in bfloat16 or wider.
A program may use at most 768 MiB of HBM per device.

```python
import jax
import jax.numpy as jnp
from jax import lax

BATCH = 8
SEQ_LEN = 512
D_MODEL = 4096
HEADS = 32
KV_HEADS = 32
HEAD_DIM = 128
D_FF = 11008
RANK = 32
ADAPTERS = 4
LORA_ALPHA = 16
RMS_EPS = 1e-5
Q_WIDTH = HEADS * HEAD_DIM
KV_WIDTH = KV_HEADS * HEAD_DIM


def draw_normal(rng_key, arr_shape, w_std):
    return (jax.random.normal(rng_key, arr_shape, jnp.float32) * w_std).astype(jnp.bfloat16)


def lora_pair(rng_key, a_shape, b_shape, fan_in, w_gain):
    key_a, key_b = jax.random.split(rng_key)
    a_stack = draw_normal(key_a, a_shape, fan_in ** -0.5)
    b_stack = draw_normal(key_b, b_shape, 0.2 * w_gain * RANK ** 0.5 / LORA_ALPHA)
    return a_stack, b_stack


def draw_ids(rng_key):
    key_perm, key_fill, key_mix = jax.random.split(rng_key, 3)
    id_perm = jax.random.permutation(key_perm, ADAPTERS).astype(jnp.int32)
    id_fill = jax.random.randint(key_fill, (BATCH,), 0, ADAPTERS).astype(jnp.int32)
    id_all = jnp.concatenate([id_perm, id_fill])[:BATCH]
    return jax.random.permutation(key_mix, id_all).astype(jnp.int32)


def setup_inputs(seed: int = 0, part: int = 0) -> dict:
    root_key = jax.random.key(seed)
    key_x, key_ids = jax.random.split(jax.random.fold_in(root_key, part))
    shared_keys = jax.random.split(root_key, 16)
    x_in = (0.5 * jax.random.normal(key_x, (BATCH, SEQ_LEN, D_MODEL), jnp.float32)).astype(jnp.bfloat16)
    gain_attn = 1.0 + 0.2 * jax.random.normal(shared_keys[0], (D_MODEL,), jnp.float32)
    gain_mlp = 1.0 + 0.2 * jax.random.normal(shared_keys[1], (D_MODEL,), jnp.float32)
    w_q = draw_normal(shared_keys[2], (D_MODEL, HEADS, HEAD_DIM), 1.7 * D_MODEL ** -0.5)
    w_k = draw_normal(shared_keys[3], (D_MODEL, KV_HEADS, HEAD_DIM), 1.7 * D_MODEL ** -0.5)
    w_v = draw_normal(shared_keys[4], (D_MODEL, KV_HEADS, HEAD_DIM), D_MODEL ** -0.5)
    w_o = draw_normal(shared_keys[5], (HEADS, HEAD_DIM, D_MODEL), Q_WIDTH ** -0.5)
    w_gate = draw_normal(shared_keys[6], (D_MODEL, D_FF), D_MODEL ** -0.5)
    w_up = draw_normal(shared_keys[7], (D_MODEL, D_FF), D_MODEL ** -0.5)
    w_down = draw_normal(shared_keys[8], (D_FF, D_MODEL), D_FF ** -0.5)
    a_q, b_q = lora_pair(shared_keys[9], (ADAPTERS, D_MODEL, RANK), (ADAPTERS, RANK, HEADS, HEAD_DIM), D_MODEL, 1.7)
    a_k, b_k = lora_pair(shared_keys[10], (ADAPTERS, D_MODEL, RANK), (ADAPTERS, RANK, KV_HEADS, HEAD_DIM), D_MODEL, 1.7)
    a_v, b_v = lora_pair(shared_keys[11], (ADAPTERS, D_MODEL, RANK), (ADAPTERS, RANK, KV_HEADS, HEAD_DIM), D_MODEL, 1.0)
    a_o, b_o = lora_pair(shared_keys[12], (ADAPTERS, HEADS, HEAD_DIM, RANK), (ADAPTERS, RANK, D_MODEL), Q_WIDTH, 1.0)
    a_gate, b_gate = lora_pair(shared_keys[13], (ADAPTERS, D_MODEL, RANK), (ADAPTERS, RANK, D_FF), D_MODEL, 1.0)
    a_up, b_up = lora_pair(shared_keys[14], (ADAPTERS, D_MODEL, RANK), (ADAPTERS, RANK, D_FF), D_MODEL, 1.0)
    a_down, b_down = lora_pair(shared_keys[15], (ADAPTERS, D_FF, RANK), (ADAPTERS, RANK, D_MODEL), D_FF, 1.0)
    return dict(x_in=x_in, adapter_ids=draw_ids(key_ids), gain_attn=gain_attn, gain_mlp=gain_mlp,
                w_q=w_q, w_k=w_k, w_v=w_v, w_o=w_o, w_gate=w_gate, w_up=w_up, w_down=w_down,
                a_q=a_q, b_q=b_q, a_k=a_k, b_k=b_k, a_v=a_v, b_v=b_v, a_o=a_o, b_o=b_o,
                a_gate=a_gate, b_gate=b_gate, a_up=a_up, b_up=b_up, a_down=a_down, b_down=b_down)


def rms_scale(x_in, gain_vec):
    x_f32 = x_in.astype(jnp.float32)
    inv_rms = lax.rsqrt(jnp.mean(x_f32 * x_f32, axis=-1, keepdims=True) + RMS_EPS)
    return (x_f32 * inv_rms * gain_vec).astype(jnp.bfloat16)


def lora_proj(h_in, w_base, a_sel, b_sel):
    base_out = jnp.dot(h_in, w_base, preferred_element_type=jnp.float32)
    lora_mid = jnp.dot(h_in, a_sel, preferred_element_type=jnp.float32).astype(jnp.bfloat16)
    return base_out + (LORA_ALPHA / RANK) * jnp.dot(lora_mid, b_sel, preferred_element_type=jnp.float32)


def attend_head(head_item):
    q_head, k_head, v_head = head_item
    scores = jnp.dot(q_head, k_head.T, preferred_element_type=jnp.float32) * HEAD_DIM ** -0.5
    causal = jnp.arange(SEQ_LEN)[:, None] >= jnp.arange(SEQ_LEN)[None, :]
    prob_bf = jax.nn.softmax(jnp.where(causal, scores, -jnp.inf), axis=-1).astype(jnp.bfloat16)
    return jnp.dot(prob_bf, v_head, preferred_element_type=jnp.float32).astype(jnp.bfloat16)


def reference(x_in, adapter_ids, gain_attn, gain_mlp, w_q, w_k, w_v, w_o, w_gate, w_up, w_down,
              a_q, b_q, a_k, b_k, a_v, b_v, a_o, b_o, a_gate, b_gate, a_up, b_up, a_down, b_down):
    head_group = HEADS // KV_HEADS
    w_query = w_q.reshape(D_MODEL, Q_WIDTH)
    w_key = w_k.reshape(D_MODEL, KV_WIDTH)
    w_value = w_v.reshape(D_MODEL, KV_WIDTH)
    w_out = w_o.reshape(Q_WIDTH, D_MODEL)

    def one_sequence(seq_item):
        x_seq, adapter_id = seq_item
        h_norm = rms_scale(x_seq, gain_attn)
        q_all = lora_proj(h_norm, w_query, a_q[adapter_id], b_q[adapter_id].reshape(RANK, Q_WIDTH)).astype(jnp.bfloat16)
        k_all = lora_proj(h_norm, w_key, a_k[adapter_id], b_k[adapter_id].reshape(RANK, KV_WIDTH)).astype(jnp.bfloat16)
        v_all = lora_proj(h_norm, w_value, a_v[adapter_id], b_v[adapter_id].reshape(RANK, KV_WIDTH)).astype(jnp.bfloat16)
        q_heads = q_all.reshape(SEQ_LEN, HEADS, HEAD_DIM).transpose(1, 0, 2)
        k_heads = jnp.repeat(k_all.reshape(SEQ_LEN, KV_HEADS, HEAD_DIM).transpose(1, 0, 2), head_group, axis=0)
        v_heads = jnp.repeat(v_all.reshape(SEQ_LEN, KV_HEADS, HEAD_DIM).transpose(1, 0, 2), head_group, axis=0)
        att_heads = lax.map(attend_head, (q_heads, k_heads, v_heads))
        att_flat = att_heads.transpose(1, 0, 2).reshape(SEQ_LEN, Q_WIDTH)
        z_out = lora_proj(att_flat, w_out, a_o[adapter_id].reshape(Q_WIDTH, RANK), b_o[adapter_id])
        x_one = (x_seq.astype(jnp.float32) + z_out).astype(jnp.bfloat16)
        h_two = rms_scale(x_one, gain_mlp)
        z_gate = lora_proj(h_two, w_gate, a_gate[adapter_id], b_gate[adapter_id]).astype(jnp.bfloat16)
        z_up = lora_proj(h_two, w_up, a_up[adapter_id], b_up[adapter_id]).astype(jnp.bfloat16)
        mlp_mid = (jax.nn.silu(z_gate.astype(jnp.float32)) * z_up.astype(jnp.float32)).astype(jnp.bfloat16)
        z_down = lora_proj(mlp_mid, w_down, a_down[adapter_id], b_down[adapter_id])
        return (x_one.astype(jnp.float32) + z_down).astype(jnp.bfloat16)

    return lax.map(one_sequence, (x_in, adapter_ids))
```

```python
import functools

import jax
import jax.numpy as jnp
from jax import lax
from jax.experimental import pallas as pl
from jax.experimental.pallas import tpu as pltpu
from jax.sharding import PartitionSpec as P

LORA_ALPHA = 16
RMS_EPS = 1e-5
LANES = 128
CORES = 2
MESH = pl.DeviceIdType.MESH
PATTERNS = (('x', 'y', 1), ('x', 'y', -1), ('y', 'x', 1), ('y', 'x', -1))
RS_PARTS = (0, 1, 2, 3, 0)


class Torus:
    def __init__(self, side):
        me = lax.axis_index('tp')
        self.side = side
        self.core = lax.rem(me, CORES)
        self.x = lax.rem(me // CORES, side)
        self.y = me // (CORES * side)

    def pos(self, axis, step=0):
        here = self.x if axis == 'x' else self.y
        return lax.rem(here + (step + self.side), self.side)

    def dev(self, axis, step):
        row, col = (self.y, self.pos('x', step)) if axis == 'x' else (self.pos('y', step), self.x)
        return {'tp': (row * self.side + col) * CORES + self.core}

    def partner(self):
        return {'tp': (self.y * self.side + self.x) * CORES + 1 - self.core}

    def barrier(self):
        sem = pltpu.get_barrier_semaphore()
        others = [self.dev(axis, step) for axis in ('x', 'y') for step in (1, -1)] + [self.partner()]
        for other in others:
            pl.semaphore_signal(sem, inc=1, device_id=other, device_id_type=MESH)
        pl.semaphore_wait(sem, len(others))


def remote(src, dst, send_sem, recv_sem, device):
    return pltpu.make_async_remote_copy(src_ref=src, dst_ref=dst, send_sem=send_sem, recv_sem=recv_sem,
                                        device_id=device, device_id_type=MESH)


def along(ref, axis, index, cols):
    return ref.at[:, index, :, cols] if axis == 'x' else ref.at[index, :, :, cols]


class ReduceScatter:
    def __init__(self, torus, parts, far, near, run, far2, near2, run2, send_sems, recv_sems):
        self.t, self.parts = torus, parts
        self.one, self.two = (far, near, run), (far2, near2, run2)
        self.send_sems, self.recv_sems = send_sems, recv_sems

    def _own(self, q, step):
        first, _, sign = PATTERNS[RS_PARTS[q]]
        ref, col, _, width = self.parts[q]
        return along(ref, first, self.t.pos(first, step * sign), pl.ds(col, width))

    def _copy(self, q, stage, kind):
        first, second, sign = PATTERNS[RS_PARTS[q]]
        _, _, col, width = self.parts[q]
        cols = pl.ds(col, width)
        axis = first if stage == 0 else second
        slots = self.one if stage == 0 else self.two
        ahead = kind != 1
        if kind == 2:
            src = slots[0]
            src = src.at[:, :, cols] if stage == 0 else src.at[:, cols]
        elif stage == 0:
            src = self._own(q, 2 if kind == 0 else -1)
        else:
            src = self.one[2].at[self.t.pos(second, (2 if kind == 0 else -1) * sign), :, cols]
        dst = slots[kind]
        dst = dst.at[:, :, cols] if stage == 0 else dst.at[:, cols]
        index = (q * 2 + stage) * 3 + kind
        return remote(src, dst, self.send_sems.at[index], self.recv_sems.at[index],
                      self.t.dev(axis, sign if ahead else -sign))

    def begin(self, q):
        self._copy(q, 0, 0).start()
        self._copy(q, 0, 1).start()

    def relay(self, q):
        self._copy(q, 0, 0).wait_recv()
        _, _, col, width = self.parts[q]
        cols = pl.ds(col, width)
        far = self.one[0]
        far[:, :, cols] = (far[:, :, cols].astype(jnp.float32) + self._own(q, 1)[...].astype(jnp.float32)).astype(far.dtype)
        self._copy(q, 0, 2).start()

    def turn(self, q):
        self._copy(q, 0, 1).wait_recv()
        self._copy(q, 0, 2).wait_recv()
        _, _, col, width = self.parts[q]
        cols = pl.ds(col, width)
        _, near, run = self.one
        total = run[:, :, cols].astype(jnp.float32) + near[:, :, cols].astype(jnp.float32)
        run[:, :, cols] = (total + self._own(q, 0)[...].astype(jnp.float32)).astype(run.dtype)
        self._copy(q, 1, 0).start()
        self._copy(q, 1, 1).start()

    def relay_two(self, q):
        _, second, sign = PATTERNS[RS_PARTS[q]]
        self._copy(q, 1, 0).wait_recv()
        _, _, col, width = self.parts[q]
        cols = pl.ds(col, width)
        far = self.two[0]
        own = self.one[2][self.t.pos(second, sign), :, cols]
        far[:, cols] = (far[:, cols].astype(jnp.float32) + own.astype(jnp.float32)).astype(far.dtype)
        self._copy(q, 1, 2).start()

    def total(self, q):
        _, second, _ = PATTERNS[RS_PARTS[q]]
        self._copy(q, 1, 1).wait_recv()
        self._copy(q, 1, 2).wait_recv()
        _, _, col, width = self.parts[q]
        cols = pl.ds(col, width)
        _, near, run = self.two
        own = self.one[2][self.t.pos(second), :, cols]
        return run[:, cols].astype(jnp.float32) + near[:, cols].astype(jnp.float32) + own.astype(jnp.float32)

    def drain(self, q):
        for stage in range(2):
            for kind in range(3):
                self._copy(q, stage, kind).wait_send()


class AllGather:
    def __init__(self, torus, buf, send_sems, recv_sems):
        self.t, self.buf = torus, buf
        self.send_sems, self.recv_sems = send_sems, recv_sems
        self.width = buf.shape[3] // len(PATTERNS)

    def _copy(self, q, inst, kind, receive=False):
        first, second, sign = PATTERNS[q]
        axis = first if inst == 0 else second
        offset = {first: 0 if inst == 0 else inst - 1, second: 0}
        if receive:
            offset[axis] = (-sign, sign, -2 * sign)[kind]
        elif kind == 2:
            offset[axis] = -sign
        piece = self.buf.at[self.t.pos('y', offset['y']), self.t.pos('x', offset['x']), :, pl.ds(q * self.width, self.width)]
        index = (q * (self.t.side + 1) + inst) * 3 + kind
        return remote(piece, piece, self.send_sems.at[index], self.recv_sems.at[index],
                      self.t.dev(axis, -sign if kind == 1 else sign))

    def _start(self, q, inst):
        self._copy(q, inst, 0).start()
        self._copy(q, inst, 1).start()

    def begin(self, q):
        self._start(q, 0)
        self._start(q, 1)

    def near(self, q):
        sign = PATTERNS[q][2]
        self._copy(q, 0, 0, True).wait_recv()
        self._copy(q, 0, 2).start()
        self._start(q, 1 + (-sign) % self.t.side)
        self._copy(q, 0, 1, True).wait_recv()
        self._start(q, 1 + sign % self.t.side)

    def far(self, q):
        self._copy(q, 0, 2, True).wait_recv()
        self._start(q, 1 + 2)

    def relay(self, q, j):
        self._copy(q, 1 + j, 0, True).wait_recv()
        self._copy(q, 1 + j, 2).start()

    def finish(self, q, j):
        self._copy(q, 1 + j, 1, True).wait_recv()
        self._copy(q, 1 + j, 2, True).wait_recv()

    def drain(self, q):
        for inst in range(self.t.side + 1):
            for kind in range(3):
                self._copy(q, inst, kind).wait_send()


NQ = len(PATTERNS)
NP = len(RS_PARTS)


def rs_kernel(side, part_hbm, rank_hbm, sum_ref, rank_sum_ref, part, rank, other, other_rank, far, near, run, far2, near2, run2,
              load_sems, pair_sems, send_sems, recv_sems):
    t = Torus(side)
    rounds, width = part.shape[0], part.shape[-1]
    share = width // NQ
    t.barrier()

    def loads(r):
        return (pltpu.make_async_copy(part_hbm.at[t.core, r], part.at[r], load_sems.at[0, r]),
                pltpu.make_async_copy(rank_hbm.at[t.core, r], rank.at[r], load_sems.at[1, r]),
                remote(part_hbm.at[1 - t.core, r], other.at[r], pair_sems.at[0, r], pair_sems.at[1, r], t.partner()),
                remote(rank_hbm.at[1 - t.core, r], other_rank.at[r], pair_sems.at[2, r], pair_sems.at[3, r], t.partner()))

    for r in range(rounds):
        for copy in loads(r):
            copy.start()

    def round_of(r):
        parts = [(part.at[r], q * share, q * share, share) for q in range(NQ)]
        parts.append((rank.at[r], 0, width, rank.shape[-1]))
        return ReduceScatter(t, parts, far.at[r], near.at[r], run.at[r], far2.at[r], near2.at[r], run2.at[r],
                             send_sems.at[r], recv_sems.at[r])

    rs = [round_of(r) for r in range(rounds)]

    def start(r):
        own, own_rank, pair, pair_rank = loads(r)
        own.wait()
        pair.wait_recv()
        own_rank.wait()
        pair_rank.wait_recv()

        @pl.loop(0, side)
        def _(i):
            for ref, more in ((part, other), (rank, other_rank)):
                ref[r, i] = (ref[r, i].astype(jnp.float32) + more[r, i].astype(jnp.float32)).astype(ref.dtype)

        for q in range(NP):
            rs[r].begin(q)

    def each(method, r):
        for q in range(NP):
            getattr(rs[r], method)(q)

    def finish(r):
        for q in range(NQ):
            sum_ref[r, :, pl.ds(q * share, share)] = rs[r].total(q)
        rank_sum_ref[r] = rs[r].total(NQ)

    start(0)
    for r in range(rounds):
        if r + 1 < rounds:
            start(r + 1)
        each('relay', r)
        if r > 0:
            each('relay_two', r - 1)
        each('turn', r)
        if r > 0:
            finish(r - 1)
    each('relay_two', rounds - 1)
    finish(rounds - 1)
    for r in range(rounds):
        each('drain', r)
        for copy in loads(r)[2:]:
            copy.wait_send()


def reduce_scatter(part, rank, side):
    cores, rounds, tokens, width = part.shape
    lanes = rank.shape[-1]
    rows = tokens // (side * side)
    dtype = part.dtype
    grid4 = (side, side, rows)
    scratch = [pltpu.VMEM((rounds,) + grid4 + (width,), dtype), pltpu.VMEM((rounds,) + grid4 + (lanes,), dtype)] * 2
    scratch += [pltpu.VMEM((rounds, side, rows, width + lanes), dtype)] * 3
    scratch += [pltpu.VMEM((rounds, rows, width + lanes), dtype)] * 3
    sems = NP * 6
    scratch += [pltpu.SemaphoreType.DMA((2, rounds)), pltpu.SemaphoreType.DMA((4, rounds)),
                pltpu.SemaphoreType.DMA((rounds, sems)), pltpu.SemaphoreType.DMA((rounds, sems))]
    return pl.pallas_call(
        functools.partial(rs_kernel, side),
        out_shape=(jax.ShapeDtypeStruct((rounds, rows, width), jnp.float32),
                   jax.ShapeDtypeStruct((rounds, rows, lanes), jnp.float32)),
        in_specs=[pl.BlockSpec(memory_space=pl.ANY)] * 2,
        out_specs=(pl.BlockSpec(memory_space=pltpu.VMEM),) * 2,
        scratch_shapes=scratch,
        compiler_params=pltpu.CompilerParams(collective_id=0, has_side_effects=True, vmem_limit_bytes=64 * 1024 * 1024 - 65536),
        name='reduce_scatter_tokens',
    )(part.reshape((cores, rounds) + grid4 + (width,)), rank.reshape((cores, rounds) + grid4 + (lanes,)))


def ag_kernel(side, shard_hbm, out_hbm, buf, load_sems, store_sems, pair_sems, send_sems, recv_sems):
    t = Torus(side)
    rounds = buf.shape[0]
    t.barrier()

    def load(r):
        return pltpu.make_async_copy(shard_hbm.at[r], buf.at[r, t.y, t.x], load_sems.at[r])

    def store(r):
        return pltpu.make_async_copy(buf.at[r], out_hbm.at[t.core, r], store_sems.at[r])

    def pair(r):
        return remote(buf.at[r], out_hbm.at[t.core, r], pair_sems.at[0, r], pair_sems.at[1, r], t.partner())

    def pair_in(r):
        return remote(buf.at[r], out_hbm.at[1 - t.core, r], pair_sems.at[0, r], pair_sems.at[1, r], t.partner())

    for r in range(rounds):
        load(r).start()
    ag = [AllGather(t, buf.at[r], send_sems.at[r], recv_sems.at[r]) for r in range(rounds)]

    def begin(r):
        load(r).wait()
        for q in range(NQ):
            ag[r].begin(q)

    begin(0)
    begin(1)
    for r in range(rounds):
        for q in range(NQ):
            ag[r].near(q)
        for q in range(NQ):
            ag[r].far(q)
        if r + 2 < rounds:
            begin(r + 2)
        for j in (0, 1, 3, 2):
            for q in range(NQ):
                ag[r].relay(q, j)
        for j in (0, 1, 3, 2):
            for q in range(NQ):
                ag[r].finish(q, j)
        store(r).start()
        pair(r).start()
    for r in range(rounds):
        for q in range(NQ):
            ag[r].drain(q)
        store(r).wait()
        pair(r).wait_send()
        pair_in(r).wait_recv()


def all_gather(shard, side):
    rounds, rows, width = shard.shape
    grid4 = (side, side, rows)
    sems = NQ * (side + 1) * 3
    out = pl.pallas_call(
        functools.partial(ag_kernel, side),
        out_shape=jax.ShapeDtypeStruct((CORES, rounds) + grid4 + (width,), shard.dtype),
        in_specs=[pl.BlockSpec(memory_space=pl.ANY)],
        out_specs=pl.BlockSpec(memory_space=pl.ANY),
        scratch_shapes=[pltpu.VMEM((rounds,) + grid4 + (width,), shard.dtype), pltpu.SemaphoreType.DMA((rounds,)),
                        pltpu.SemaphoreType.DMA((rounds,)), pltpu.SemaphoreType.DMA((2, rounds)),
                        pltpu.SemaphoreType.DMA((rounds, sems)), pltpu.SemaphoreType.DMA((rounds, sems))],
        compiler_params=pltpu.CompilerParams(collective_id=1, has_side_effects=True, vmem_limit_bytes=64 * 1024 * 1024 - 65536),
        name='all_gather_tokens',
    )(shard)
    return out.reshape(CORES, rounds, side * side * rows, width)


def rms_scale(x_in, gain_vec):
    x_f32 = x_in.astype(jnp.float32)
    inv_rms = lax.rsqrt(jnp.mean(x_f32 * x_f32, axis=-1, keepdims=True) + RMS_EPS)
    return (x_f32 * inv_rms * gain_vec).astype(jnp.bfloat16)


def causal_attention(q_flat, k_flat, v_flat, kv_heads, head_dim):
    num_seqs, seq_len = q_flat.shape[0], q_flat.shape[1]
    q_group = q_flat.reshape(num_seqs, seq_len, kv_heads, -1, head_dim)
    k_group = k_flat.reshape(num_seqs, seq_len, kv_heads, head_dim)
    v_group = v_flat.reshape(num_seqs, seq_len, kv_heads, head_dim)
    scores = jnp.einsum('bqngd,bknd->bngqk', q_group, k_group, preferred_element_type=jnp.float32) * head_dim ** -0.5
    causal = jnp.arange(seq_len)[:, None] >= jnp.arange(seq_len)[None, :]
    prob_bf = jax.nn.softmax(jnp.where(causal, scores, -jnp.inf), axis=-1).astype(jnp.bfloat16)
    att_out = jnp.einsum('bngqk,bknd->bqngd', prob_bf, v_group, preferred_element_type=jnp.float32)
    return att_out.astype(jnp.bfloat16).reshape(num_seqs, seq_len, -1)


def solution(mesh):
    act_spec = P('dp', None, None)
    w_head_spec = P(None, 'tp', None)
    w_out_spec = P('tp', None, None)
    w_col_spec = P(None, 'tp')
    w_row_spec = P('tp', None)
    a_rank_spec = P(None, None, 'tp')
    b_head_spec = P(None, None, 'tp', None)
    b_col_spec = P(None, None, 'tp')
    a_head_spec = P(None, 'tp', None, None)
    a_row_spec = P(None, 'tp', None)
    in_specs = (act_spec, P('dp'), P(None), P(None), w_head_spec, w_head_spec, w_head_spec, w_out_spec,
                w_col_spec, w_col_spec, w_row_spec, a_rank_spec, b_head_spec, a_rank_spec, b_head_spec,
                a_rank_spec, b_head_spec, a_head_spec, b_col_spec, a_rank_spec, b_col_spec,
                a_rank_spec, b_col_spec, a_row_spec, b_col_spec)
    devices = mesh.shape['tp']
    side = round((devices // CORES) ** 0.5)

    def local_layer(x_in, adapter_ids, gain_attn, gain_mlp, w_q, w_k, w_v, w_o, w_gate, w_up, w_down,
                    a_q, b_q, a_k, b_k, a_v, b_v, a_o, b_o, a_gate, b_gate, a_up, b_up, a_down, b_down):
        num_seqs, seq_len, model_dim = x_in.shape
        rank = b_q.shape[1]
        scale = LORA_ALPHA / rank
        rounds = num_seqs // CORES
        rows = seq_len // (devices // CORES)
        me = lax.axis_index('tp')
        core, chip = me % CORES, me // CORES

        a_mine = jnp.stack([a_q, a_k, a_v, a_gate, a_up]).reshape(5, -1, model_dim).transpose(1, 0, 2)
        b_mine = jnp.stack([b_o, b_down]).transpose(1, 2, 0, 3)
        a_all = lax.all_gather(a_mine, 'tp', axis=2, tiled=False)
        b_all = lax.all_gather(b_mine, 'tp', axis=3, tiled=True)

        def per_sequence(stack):
            return jnp.take(stack, adapter_ids, axis=0)

        a_seq = per_sequence(a_all)

        def column(h_in, w_locs, which, b_stacks):
            a_sel = a_seq[:, which[0]:which[1]].reshape(num_seqs, -1, model_dim)
            mid = jnp.einsum('bsd,brd->bsr', h_in, a_sel, preferred_element_type=jnp.float32).astype(jnp.bfloat16)
            outs = []
            for i, (w_loc, b_stack) in enumerate(zip(w_locs, b_stacks)):
                base = jnp.einsum('bsd,de->bse', h_in, w_loc.reshape(model_dim, -1), preferred_element_type=jnp.float32)
                low = jnp.einsum('bsr,bre->bse', mid[:, :, i * rank:(i + 1) * rank],
                                 per_sequence(b_stack).reshape(num_seqs, rank, -1), preferred_element_type=jnp.float32)
                outs.append((base + scale * low).astype(jnp.bfloat16))
            return outs

        def mine(full):
            rows_of = full.reshape((CORES, rounds, devices // CORES, rows) + full.shape[2:])
            rows_of = lax.dynamic_slice_in_dim(rows_of, core, 1, axis=0)[0]
            return lax.dynamic_slice_in_dim(rows_of, chip, 1, axis=1)[:, 0]

        def row_proj(h_in, w_loc, a_stack, b_full, resid):
            part = jnp.einsum('bse,ed->bsd', h_in, w_loc, preferred_element_type=jnp.float32).astype(jnp.bfloat16)
            mid = jnp.einsum('bse,ber->bsr', h_in, per_sequence(a_stack).reshape(num_seqs, -1, rank),
                             preferred_element_type=jnp.float32).astype(jnp.bfloat16)
            mid = jnp.pad(mid, ((0, 0), (0, 0), (0, LANES - rank)))
            split = (CORES, rounds, seq_len)
            total, mid_total = reduce_scatter(part.reshape(split + (model_dim,)), mid.reshape(split + (LANES,)), side)
            ids = lax.dynamic_slice_in_dim(adapter_ids, core * rounds, rounds, axis=0)
            low = jnp.einsum('bsr,brd->bsd', mid_total[:, :, :rank].astype(jnp.bfloat16), jnp.take(b_full, ids, axis=0),
                             preferred_element_type=jnp.float32)
            return (resid.astype(jnp.float32) + (total + scale * low)).astype(jnp.bfloat16)

        def whole(shard):
            return all_gather(shard, side).reshape(num_seqs, seq_len, model_dim)

        h_norm = rms_scale(x_in, gain_attn)
        q_loc, k_loc, v_loc = column(h_norm, (w_q, w_k, w_v), (0, 3), (b_q, b_k, b_v))
        att_loc = causal_attention(q_loc, k_loc, v_loc, w_k.shape[1], w_k.shape[2])
        x_one = row_proj(att_loc, w_o.reshape(-1, model_dim), a_o, b_all[:, :, 0], mine(x_in))
        h_two = whole(rms_scale(x_one, gain_mlp))
        gate_loc, up_loc = column(h_two, (w_gate, w_up), (3, 5), (b_gate, b_up))
        mlp_mid = (jax.nn.silu(gate_loc.astype(jnp.float32)) * up_loc.astype(jnp.float32)).astype(jnp.bfloat16)
        return whole(row_proj(mlp_mid, w_down, a_down, b_all[:, :, 1], x_one))

    return jax.shard_map(local_layer, mesh=mesh, in_specs=in_specs, out_specs=act_spec, check_vma=False)
```
